256 devices in a mesh: row: 16 (over x_hi, z), col: 16 (over x_lo, y, core).
Axes of the slice: x: 4 (x_hi: 2, x_lo: 2; x = x_hi * 2 + x_lo), y: 4, z: 8, core: 2. Of those that a mesh axis runs over, the one named last changes fastest.
Arguments:
- pair: bfloat16 [512, 512, 128], P('row', 'col'), may hold values from -6 to 6
- norm_in: float32 [128], replicated, may hold values from 0.1 to 1.9
- shift_in: float32 [128], replicated, may hold values from -3 to 3
- in_weight: bfloat16 [128, 640], replicated, may hold values from -0.5 to 0.5
- norm_out: float32 [128], replicated, may hold values from 0.1 to 1.9
- shift_out: float32 [128], replicated, may hold values from -3 to 3
- out_weight: bfloat16 [128, 128], replicated, may hold values from -0.5 to 0.5
Outputs:
- update: bfloat16 [512, 512, 128], P('row', 'col')
The draws below stay inside these ranges and needn't reach their ends.
All inputs are finite; a program needn't handle non-finite values.
Results may differ from the reference program's by a relative error of at most 0.0054.
Values may be sent and summed in bfloat16 or wider, within the bound.
A program may use at most 64 MiB of HBM per device.

```python
import jax
import jax.numpy as jnp
from jax import lax

C = 128
CH = 128
N = 512
ROWS = 32
N_ROW = 16


def block_levels(key, extent, split, smallest, high):
    loudness, own = 1.0, jax.random.fold_in(key, 6)
    for dim, blocks in split:
        heights = jnp.exp(jax.random.uniform(jax.random.fold_in(own, dim), (blocks,), jnp.float32, smallest / len(split), high / len(split)))
        loudness = loudness * jnp.repeat(heights, extent[dim] // blocks).reshape([-1 if axis == dim else 1 for axis in range(len(extent))])
    return loudness


def centred(key, extent, scale, bound, pieces=(), held_as=jnp.bfloat16):
    result = jax.random.normal(key, extent, jnp.float32) * scale
    if len(pieces) > 0:
        result = block_levels(key, extent, pieces, -0.22, 0.18) * result
    return jnp.clip(result, min=-bound, max=bound).astype(held_as)


def setup_inputs(seed: int = 0) -> dict:
    streams_of = jax.random.split(jax.random.key(seed), 8)
    return {
        "pair": centred(streams_of[0], (N, N, C), 1.0, 6.0, ((0, 16), (1, 16))),
        "norm_in": jnp.clip(1.0 + 0.18 * jax.random.normal(streams_of[1], (C,), jnp.float32), 0.1, 1.9),
        "shift_in": centred(streams_of[2], (C,), 0.5, 3.0, (), jnp.float32),
        "in_weight": centred(streams_of[3], (C, 4 * CH + C), C ** -0.5, 0.5),
        "norm_out": jnp.clip(1.0 + 0.18 * jax.random.normal(streams_of[4], (CH,), jnp.float32), 0.1, 1.9),
        "shift_out": centred(streams_of[5], (CH,), 0.5, 3.0, (), jnp.float32),
        "out_weight": centred(streams_of[6], (CH, C), CH ** -0.5, 0.5),
    }


EPSILON = 1e-05

def layer_norm(values, gain, shift):
    values = values.astype(jnp.float32)
    center = lax.optimization_barrier(jnp.mean(values, axis=-1, keepdims=True))
    spread = lax.optimization_barrier(jnp.mean(jnp.square(values - center), axis=-1, keepdims=True))
    return (values - center) * lax.rsqrt(spread + EPSILON) * gain + shift

def project_block(block, norm_in, shift_in, in_weight):
    normed = layer_norm(block, norm_in, shift_in).astype(jnp.bfloat16)
    projected = jnp.dot(normed.reshape(-1, C), in_weight, preferred_element_type=jnp.float32)
    left = (jax.nn.sigmoid(projected[:, :CH]) * projected[:, CH:2 * CH]).astype(jnp.bfloat16)
    right = (jax.nn.sigmoid(projected[:, 2 * CH:3 * CH]) * projected[:, 3 * CH:4 * CH]).astype(jnp.bfloat16)
    gate = jax.nn.sigmoid(projected[:, 4 * CH:])
    return (left, right, gate)

def reference(pair, norm_in, shift_in, in_weight, norm_out, shift_out, out_weight):
    blocks = pair.reshape(N_ROW, ROWS, N, C)
    left, right, gate = lax.map(lambda block: project_block(block, norm_in, shift_in, in_weight), blocks)
    left = left.reshape(N, N, CH).astype(jnp.float32)
    right = right.reshape(N, N, CH).astype(jnp.float32)
    gate = gate.reshape(N, N, C)
    mixed = jnp.einsum('kih,kjh->ijh', left, right)
    mixed_normed = layer_norm(mixed, norm_out, shift_out).astype(jnp.bfloat16)
    outward = jnp.dot(mixed_normed.reshape(-1, CH), out_weight, preferred_element_type=jnp.float32)
    return (gate * outward.reshape(N, N, C)).astype(jnp.bfloat16)
```

```python
import jax
import jax.numpy as jnp
from jax import lax
from jax.experimental import pallas as pl
from jax.experimental.pallas import tpu as pltpu
from jax.sharding import PartitionSpec as P

EPSILON = 1e-05
MESH = pl.DeviceIdType.MESH
PITCH = 40
NT = (((1,), (1,)), ((), ()))
TN = (((0,), (0,)), ((), ()))


def z_step(t):
    return 4 + (1 - 2 * (t % 2)) * ((t + 1) // 2)


def y_step(u):
    return 2 + (1 - 2 * lax.rem(u, 2)) * lax.div(u + 1, 2)


def swap_blocks(tiles):
    lane = lax.broadcasted_iota(jnp.int32, tiles[0].shape, 1)
    low, even = lane < 64, lax.rem(lax.div(lane, 32), 2) == 0

    def turn(x, shift):
        return pltpu.roll(x, shift, 1)

    a, b, c, d = tiles
    a, c = jnp.where(low, a, turn(c, 64)), jnp.where(low, turn(a, 64), c)
    b, d = jnp.where(low, b, turn(d, 64)), jnp.where(low, turn(b, 64), d)
    a, b = jnp.where(even, a, turn(b, 32)), jnp.where(even, turn(a, 96), b)
    c, d = jnp.where(even, c, turn(d, 32)), jnp.where(even, turn(c, 96), d)
    return a, b, c, d


def kernel(
    pair, norm_in, shift_in, in_weight, norm_out, shift_out, out_weight, out,
    normed, staged, sent, landed, left, right, mixed, back, gate, gain, bias, weight,
    dma, ready,
):
    f32, bf16 = jnp.float32, jnp.bfloat16
    r, c = lax.axis_index("row"), lax.axis_index("col")
    xh, z = lax.div(r, 8), lax.rem(r, 8)
    xl, y, core = lax.div(c, 8), lax.rem(lax.div(c, 2), 4), lax.rem(c, 2)
    spot = lax.div(c, 2)

    barrier = pltpu.get_barrier_semaphore()
    for s in range(1, 16):
        pl.semaphore_signal(barrier, inc=1, device_id=(lax.rem(r + s, 16), c), device_id_type=MESH)
    for s in range(1, 16):
        pl.semaphore_signal(barrier, inc=1, device_id=(r, lax.rem(c + s, 16)), device_id_type=MESH)

    def norm_rows(n, _):
        x = pair[pl.ds(n * 128, 128), :].astype(f32)
        center = jnp.mean(x, axis=-1, keepdims=True)
        x = x - center
        spread = jnp.mean(x * x, axis=-1, keepdims=True)
        x = x * lax.rsqrt(spread + EPSILON) * norm_in[...] + shift_in[...]
        for m in range(4):
            normed[pl.ds((n * 4 + m) * PITCH, 32), :] = x[m * 32 : (m + 1) * 32]
        return 0

    lax.fori_loop(0, 8, norm_rows, 0)
    weight[...] = in_weight[:, :512].astype(f32).T.astype(bf16)

    def glu(rows, x):
        p = lax.dot_general(weight[pl.ds(rows, 256), :], x, NT, preferred_element_type=f32)
        return jax.nn.sigmoid(p[:128]) * p[128:]

    for s in range(0, 8, 2):
        parts = [normed[pl.ds(b * 8 + s + e, 32, stride=PITCH), :] for e in range(2) for b in range(4)]
        value = glu(0, jnp.concatenate(parts, axis=0).astype(bf16))
        for e in range(2):
            staged[pl.ds(s + e, 128, stride=16), :] = value[:, e * 128 : (e + 1) * 128]
        parts = [normed[pl.ds((b * 8 + s + e) * PITCH, 32), :] for e in range(2) for b in range(4)]
        value = glu(256, jnp.concatenate(parts, axis=0).astype(bf16))
        for e in range(2):
            staged[pl.ds(8 + s + e, 128, stride=16), :] = value[:, e * 128 : (e + 1) * 128]

    def pack(n, _):
        sent[pl.ds(n * 16, 16)] = staged[pl.ds(n * 256, 256), :].astype(bf16).reshape(16, 16, 128)
        return 0

    lax.fori_loop(0, 8, pack, 0)

    pl.semaphore_wait(barrier, 30)
    for s in range(1, 16):
        pl.semaphore_signal(ready, inc=1, device_id=(r, lax.rem(c + s, 16)), device_id_type=MESH)
    pl.semaphore_wait(ready, 15)

    def inward(R, S, send):
        return pltpu.make_async_remote_copy(
            src_ref=sent.at[R * 8 + S], dst_ref=landed.at[r, lax.rem(c, 8)], send_sem=dma.at[send],
            recv_sem=dma.at[1], device_id=(R, S * 2 + xl), device_id_type=MESH,
        )

    for t in range(8):
        def go_in(s, _, t=t):
            R = lax.rem(xh + 1 - lax.div(s, 8), 2) * 8 + lax.rem(z + z_step(t), 8)
            S = lax.rem(xl + 1 - lax.rem(lax.div(s, 4), 2), 2) * 4 + lax.rem(y + y_step(lax.rem(s, 4)), 4)
            inward(R, S, 0).start()
            return 0

        lax.fori_loop(0, 16 if t < 7 else 15, go_in, 0)
    own_in = pltpu.make_async_copy(sent.at[r * 8 + spot], landed.at[r, lax.rem(c, 8)], dma.at[1])
    pl.when(xl == core)(own_in.start)
    pl.when(xl != core)(inward(r, spot, 2).start)

    def gate_rows(n, _):
        parts = [normed[pl.ds((n * 4 + m) * PITCH, 32), :] for m in range(4)]
        x = jnp.concatenate(parts, axis=0).astype(bf16)
        p = jnp.dot(x, in_weight[:, 512:], preferred_element_type=f32)
        gate[pl.ds(n * 4, 4)] = jax.nn.sigmoid(p).reshape(4, 32, 128)
        return 0

    lax.fori_loop(0, 8, gate_rows, 0)
    gain[...] = jnp.broadcast_to(norm_out[...], (128, 128)).T
    bias[...] = jnp.broadcast_to(shift_out[...], (128, 128)).T

    pltpu.make_async_copy(landed, landed, dma.at[1]).wait()

    for q in range(2):
        tiles = [landed[:, q * 4 + n].astype(f32)[:, 8:].reshape(128, 128) for n in range(4)]
        tiles = [t.reshape(16, 1, 8, 128) for t in swap_blocks(tiles)]
        block = jnp.concatenate(tiles, axis=1).reshape(512, 128)
        right[0, :, q * 128 : (q + 1) * 128] = block.astype(bf16)
    for n in range(8):
        tiles = landed[:, n].astype(f32)[:, :8].reshape(4, 4, 8, 128)
        tiles = swap_blocks([tiles[:, m].reshape(32, 128) for m in range(4)])
        for m in range(4):
            block = jnp.concatenate([t[m * 8 : (m + 1) * 8] for t in tiles], axis=0)
            left[n * 32 : (n + 1) * 32, m * 128 : (m + 1) * 128] = block.astype(bf16)

    swap = pltpu.make_async_remote_copy(
        src_ref=right.at[0], dst_ref=right.at[1], send_sem=dma.at[3], recv_sem=dma.at[4],
        device_id=(r, spot * 2 + 1 - core), device_id_type=MESH,
    )
    swap.start()

    def outward(R, C, half, send):
        return pltpu.make_async_remote_copy(
            src_ref=mixed.at[lax.rem(R, 8), half, lax.rem(C, 8)], dst_ref=back.at[r * 8 + spot],
            send_sem=dma.at[send], recv_sem=dma.at[6], device_id=(R, C), device_id_type=MESH,
        )

    for half in range(2):
        if half == 1:
            swap.wait()
        product = jnp.dot(left[...], right[half], preferred_element_type=f32)
        for q in range(2):
            tiles = product[:, q * 128 : (q + 1) * 128].reshape(8, 4, 8, 128)
            tiles = swap_blocks([tiles[:, m].reshape(64, 128) for m in range(4)])
            for m in range(4):
                mixed[:, half, q * 4 + m] = tiles[m].reshape(8, 8, 128).astype(bf16)
        X = lax.rem(core + half, 2)
        for t in range(8):
            def go_out(s, _, t=t, half=half, X=X):
                R = core * 8 + lax.rem(z + z_step(t), 8)
                C = X * 8 + lax.rem(y + y_step(lax.div(s, 2)), 4) * 2 + lax.rem(core + s, 2)
                outward(R, C, half, 5).start()
                return 0

            lax.fori_loop(0, 8 if t < 7 else 6, go_out, 0)
        R, C = core * 8 + z, X * 8 + y * 2
        outward(R, C + 1 - core, half, 5).start()
        mine = (xh == core) & (xl == X)
        own_out = pltpu.make_async_copy(
            mixed.at[z, half, lax.rem(c, 8)], back.at[r * 8 + spot], dma.at[6]
        )
        pl.when(mine)(own_out.start)
        pl.when(jnp.logical_not(mine))(outward(R, C + core, half, 7 + half).start)

    pltpu.make_async_copy(back, back, dma.at[6]).wait()

    def total(n, s):
        return s + jnp.sum(back[pl.ds(n * 16, 16)].astype(f32), axis=0)

    center = lax.fori_loop(0, 8, total, jnp.zeros((8, 128), f32)) / 128

    def square(n, s):
        x = back[pl.ds(n * 16, 16)].astype(f32) - center[None]
        return s + jnp.sum(x * x, axis=0)

    scale = lax.rsqrt(lax.fori_loop(0, 8, square, jnp.zeros((8, 128), f32)) / 128 + EPSILON)

    def rescale(n, _):
        x = (back[pl.ds(n * 16, 16)].astype(f32) - center[None]) * scale[None]
        staged[pl.ds(n * 128, 128), :] = x.reshape(128, 128)
        return 0

    lax.fori_loop(0, 8, rescale, 0)
    for s in range(8):
        x = staged[pl.ds(s, 128, stride=8), :] * gain[...] + bias[...]
        x = lax.dot_general(x.astype(bf16), out_weight[...], TN, preferred_element_type=f32)
        for b in range(4):
            out[b * 8 + s] = (gate[b * 8 + s] * x[b * 32 : (b + 1) * 32]).astype(bf16)

    left_over = sent.at[pl.ds(0, 127)]
    pltpu.make_async_copy(left_over, left_over, dma.at[0]).wait()
    pl.when(xl != core)(pltpu.make_async_copy(sent.at[0], sent.at[0], dma.at[2]).wait)
    left_over = back.at[pl.ds(0, 126)]
    pltpu.make_async_copy(left_over, left_over, dma.at[5]).wait()
    for half in range(2):
        mine = (xh == core) & (xl == lax.rem(core + half, 2))
        one = pltpu.make_async_copy(back.at[0], back.at[0], dma.at[7 + half])
        pl.when(jnp.logical_not(mine))(one.wait)


def local(pair, norm_in, shift_in, in_weight, norm_out, shift_out, out_weight):
    f32, bf16 = jnp.float32, jnp.bfloat16
    vmem = pl.BlockSpec(memory_space=pltpu.VMEM)
    return pl.pallas_call(
        kernel,
        out_shape=jax.ShapeDtypeStruct((32, 32, 128), bf16),
        in_specs=[vmem] * 7,
        out_specs=vmem,
        scratch_shapes=[
            pltpu.VMEM((32 * PITCH, 128), f32),
            pltpu.VMEM((2048, 128), f32),
            pltpu.VMEM((128, 16, 128), bf16),
            pltpu.VMEM((16, 8, 16, 128), bf16),
            pltpu.VMEM((256, 512), bf16),
            pltpu.VMEM((2, 512, 256), bf16),
            pltpu.VMEM((8, 2, 8, 8, 128), bf16),
            pltpu.VMEM((128, 8, 128), bf16),
            pltpu.VMEM((32, 32, 128), f32),
            pltpu.VMEM((128, 128), f32),
            pltpu.VMEM((128, 128), f32),
            pltpu.VMEM((512, 128), bf16),
            pltpu.SemaphoreType.DMA((9,)),
            pltpu.SemaphoreType.REGULAR,
        ],
        name="triangle",
        compiler_params=pltpu.CompilerParams(collective_id=0, has_side_effects=True),
    )(
        pair.reshape(1024, 128), norm_in.reshape(1, 128), shift_in.reshape(1, 128), in_weight,
        norm_out.reshape(1, 128), shift_out.reshape(1, 128), out_weight,
    )


def solution(mesh):
    in_specs = (P("row", "col", None), P(), P(), P(), P(), P(), P())
    out_specs = P("row", "col", None)
    return jax.shard_map(local, mesh=mesh, in_specs=in_specs, out_specs=out_specs, check_vma=False)
```

```python
import jax
import jax.numpy as jnp
from jax import lax
from jax.experimental import pallas as pl
from jax.experimental.pallas import tpu as pltpu
from jax.sharding import PartitionSpec as P

EPSILON = 1e-05
MESH = pl.DeviceIdType.MESH
PITCH = 40
NT = (((1,), (1,)), ((), ()))
TN = (((0,), (0,)), ((), ()))
Y_STEP = (2, 1, 3, 0)
ORDER = (
    (0, 0), (0, 1), (0, 3), (1, 0), (3, 0), (0, 2), (1, 1), (1, 3),
    (3, 1), (3, 3), (2, 0), (1, 2), (3, 2), (2, 1), (2, 3), (2, 2),
)


def z_step(t):
    return 4 + (1 - 2 * (t % 2)) * ((t + 1) // 2)


def swap_blocks(tiles):
    lane = lax.broadcasted_iota(jnp.int32, tiles[0].shape, 1)
    low, even = lane < 64, lax.rem(lax.div(lane, 32), 2) == 0

    def turn(x, shift):
        return pltpu.roll(x, shift, 1)

    a, b, c, d = tiles
    a, c = jnp.where(low, a, turn(c, 64)), jnp.where(low, turn(a, 64), c)
    b, d = jnp.where(low, b, turn(d, 64)), jnp.where(low, turn(b, 64), d)
    a, b = jnp.where(even, a, turn(b, 32)), jnp.where(even, turn(a, 96), b)
    c, d = jnp.where(even, c, turn(d, 32)), jnp.where(even, turn(c, 96), d)
    return a, b, c, d


def kernel(
    pair_in, norm_in_in, shift_in_in, in_weight_in, norm_out_in, shift_out_in, out_weight_in, out,
    pair, norm_in, shift_in, in_weight, norm_out, shift_out, out_weight,
    normed, staged, sent, landed, left, right, mixed, back, gate, gain, bias, weight,
    dma, load, ready,
):
    f32, bf16 = jnp.float32, jnp.bfloat16
    r, c = lax.axis_index("row"), lax.axis_index("col")
    xh, z = lax.div(r, 8), lax.rem(r, 8)
    xl, y, core = lax.div(c, 8), lax.rem(lax.div(c, 2), 4), lax.rem(c, 2)
    spot = lax.div(c, 2)

    sources = (pair_in, norm_in_in, shift_in_in, in_weight_in, norm_out_in, shift_out_in, out_weight_in)
    places = (pair, norm_in, shift_in, in_weight, norm_out, shift_out, out_weight)
    loads = [pltpu.make_async_copy(f, t, load.at[n]) for n, (f, t) in enumerate(zip(sources, places))]
    for n in (0, 3, 1, 2, 4, 5, 6):
        loads[n].start()

    def line(dx, dy):
        x = lax.rem(2 * xh + xl + dx, 4)
        return lax.div(x, 2), lax.rem(x, 2) * 4 + lax.rem(y + dy, 4)

    def tell(semaphore, R, C):
        pl.semaphore_signal(semaphore, inc=1, device_id=(R, C), device_id_type=MESH)

    barrier = pltpu.get_barrier_semaphore()
    for dx, dy in ((1, 0), (3, 0), (0, 1), (0, 3)):
        H, S = line(dx, dy)
        tell(barrier, H * 8 + z, S * 2 + core)
    for dz in (4, 3, 5, 2, 6, 1, 7):
        for e in range(2):
            tell(barrier, xh * 8 + lax.rem(z + dz, 8), spot * 2 + e)
    tell(barrier, r, spot * 2 + 1 - core)

    for n in (0, 1, 2):
        loads[n].wait()

    def norm_rows(n, _):
        x = pair[pl.ds(n * 128, 128), :].astype(f32)
        center = jnp.mean(x, axis=-1, keepdims=True)
        x = x - center
        spread = jnp.mean(x * x, axis=-1, keepdims=True)
        x = x * lax.rsqrt(spread + EPSILON) * norm_in[...] + shift_in[...]
        for m in range(4):
            normed[pl.ds((n * 4 + m) * PITCH, 32), :] = x[m * 32 : (m + 1) * 32]
        return 0

    lax.fori_loop(0, 8, norm_rows, 0)
    loads[3].wait()
    weight[...] = in_weight[:, :512].astype(f32).T.astype(bf16)

    def glu(rows, x):
        p = lax.dot_general(weight[pl.ds(rows, 256), :], x, NT, preferred_element_type=f32)
        return jax.nn.sigmoid(p[:128]) * p[128:]

    for s in range(0, 8, 2):
        parts = [normed[pl.ds(b * 8 + s + e, 32, stride=PITCH), :] for e in range(2) for b in range(4)]
        value = glu(0, jnp.concatenate(parts, axis=0).astype(bf16))
        for e in range(2):
            staged[pl.ds(s + e, 128, stride=16), :] = value[:, e * 128 : (e + 1) * 128]
        parts = [normed[pl.ds((b * 8 + s + e) * PITCH, 32), :] for e in range(2) for b in range(4)]
        value = glu(256, jnp.concatenate(parts, axis=0).astype(bf16))
        for e in range(2):
            staged[pl.ds(8 + s + e, 128, stride=16), :] = value[:, e * 128 : (e + 1) * 128]

    def pack(n, _):
        sent[pl.ds(n * 16, 16)] = staged[pl.ds(n * 256, 256), :].astype(bf16).reshape(16, 16, 128)
        return 0

    lax.fori_loop(0, 8, pack, 0)

    def inward(R, S, send):
        return pltpu.make_async_remote_copy(
            src_ref=sent.at[R * 8 + S], dst_ref=landed.at[r, lax.rem(c, 8)], send_sem=dma.at[send],
            recv_sem=dma.at[1], device_id=(R, S * 2 + xl), device_id_type=MESH,
        )

    pl.semaphore_wait(barrier, 19)
    for dx, dy in ORDER:
        H, S = line(dx, dy)
        if (dx, dy) != (0, 0):
            pl.semaphore_wait(ready.at[dx * 4 + dy], 1)

        def pass_on(ex, ey, dx=dx, dy=dy):
            h, s = line(ex, ey)
            tell(ready.at[(dx - ex) % 4 * 4 + (dy - ey) % 4], h * 8 + z, s * 2 + core)

        if dx == 0:
            if dy in (0, 1):
                pass_on(0, 3)
            if dy == 0:
                pass_on(0, 1)
            pass_on(3, 0)
            pass_on(1, 0)
        if dx == 1:
            pass_on(3, 0)

        def go_in(t, _, H=H, S=S):
            inward(H * 8 + lax.rem(z + z_step(t), 8), S, 0).start()
            return 0

        lax.fori_loop(0, 7 if (dx, dy) == (0, 0) else 8, go_in, 0, unroll=True)
        if (dx, dy) == (0, 0):
            own_in = pltpu.make_async_copy(sent.at[r * 8 + spot], landed.at[r, lax.rem(c, 8)], dma.at[1])
            pl.when(xl == core)(own_in.start)
            pl.when(xl != core)(inward(r, spot, 2).start)

    def gate_rows(n, _):
        parts = [normed[pl.ds((n * 4 + m) * PITCH, 32), :] for m in range(4)]
        x = jnp.concatenate(parts, axis=0).astype(bf16)
        p = jnp.dot(x, in_weight[:, 512:], preferred_element_type=f32)
        gate[pl.ds(n * 4, 4)] = jax.nn.sigmoid(p).reshape(4, 32, 128)
        return 0

    lax.fori_loop(0, 8, gate_rows, 0)
    for n in (4, 5, 6):
        loads[n].wait()
    gain[...] = jnp.broadcast_to(norm_out[...], (128, 128)).T
    bias[...] = jnp.broadcast_to(shift_out[...], (128, 128)).T

    pltpu.make_async_copy(landed, landed, dma.at[1]).wait()

    for q in range(2):
        tiles = [landed[:, q * 4 + n].astype(f32)[:, 8:].reshape(128, 128) for n in range(4)]
        tiles = [t.reshape(16, 1, 8, 128) for t in swap_blocks(tiles)]
        block = jnp.concatenate(tiles, axis=1).reshape(512, 128)
        right[0, :, q * 128 : (q + 1) * 128] = block.astype(bf16)
    for n in range(8):
        tiles = landed[:, n].astype(f32)[:, :8].reshape(4, 4, 8, 128)
        tiles = swap_blocks([tiles[:, m].reshape(32, 128) for m in range(4)])
        for m in range(4):
            block = jnp.concatenate([t[m * 8 : (m + 1) * 8] for t in tiles], axis=0)
            left[n * 32 : (n + 1) * 32, m * 128 : (m + 1) * 128] = block.astype(bf16)

    swap = pltpu.make_async_remote_copy(
        src_ref=right.at[0], dst_ref=right.at[1], send_sem=dma.at[3], recv_sem=dma.at[4],
        device_id=(r, spot * 2 + 1 - core), device_id_type=MESH,
    )
    swap.start()

    def outward(R, C, half, send):
        return pltpu.make_async_remote_copy(
            src_ref=mixed.at[lax.rem(R, 8), half, lax.rem(C, 8)], dst_ref=back.at[r * 8 + spot],
            send_sem=dma.at[send], recv_sem=dma.at[6], device_id=(R, C), device_id_type=MESH,
        )

    for half in range(2):
        if half == 1:
            swap.wait()
        product = jnp.dot(left[...], right[half], preferred_element_type=f32)
        for q in range(2):
            tiles = product[:, q * 128 : (q + 1) * 128].reshape(8, 4, 8, 128)
            tiles = swap_blocks([tiles[:, m].reshape(64, 128) for m in range(4)])
            for m in range(4):
                mixed[:, half, q * 4 + m] = tiles[m].reshape(8, 8, 128).astype(bf16)
        X = lax.rem(core + half, 2)

        def go_out(t, _, half=half, X=X):
            R = core * 8 + lax.rem(z + z_step(t), 8)
            for u in range(4):
                for e in range(2):
                    C = X * 8 + lax.rem(y + Y_STEP[u], 4) * 2 + lax.rem(core + 1 - e, 2)
                    outward(R, C, half, 5).start()
            return 0

        lax.fori_loop(0, 7, go_out, 0)
        R, C = core * 8 + z, X * 8 + y * 2
        for u in range(3):
            for e in range(2):
                outward(R, X * 8 + lax.rem(y + Y_STEP[u], 4) * 2 + e, half, 5).start()
        outward(R, C + 1 - core, half, 5).start()
        mine = (xh == core) & (xl == X)
        own_out = pltpu.make_async_copy(
            mixed.at[z, half, lax.rem(c, 8)], back.at[r * 8 + spot], dma.at[6]
        )
        pl.when(mine)(own_out.start)
        pl.when(jnp.logical_not(mine))(outward(R, C + core, half, 7 + half).start)

    pltpu.make_async_copy(back, back, dma.at[6]).wait()

    def total(n, s):
        return s + jnp.sum(back[pl.ds(n * 16, 16)].astype(f32), axis=0)

    center = lax.fori_loop(0, 8, total, jnp.zeros((8, 128), f32)) / 128

    def square(n, s):
        x = back[pl.ds(n * 16, 16)].astype(f32) - center[None]
        return s + jnp.sum(x * x, axis=0)

    scale = lax.rsqrt(lax.fori_loop(0, 8, square, jnp.zeros((8, 128), f32)) / 128 + EPSILON)

    def rescale(n, _):
        x = (back[pl.ds(n * 16, 16)].astype(f32) - center[None]) * scale[None]
        staged[pl.ds(n * 128, 128), :] = x.reshape(128, 128)
        return 0

    lax.fori_loop(0, 8, rescale, 0)
    for s in range(8):
        x = staged[pl.ds(s, 128, stride=8), :] * gain[...] + bias[...]
        x = lax.dot_general(x.astype(bf16), out_weight[...], TN, preferred_element_type=f32)
        for b in range(4):
            out[b * 8 + s] = (gate[b * 8 + s] * x[b * 32 : (b + 1) * 32]).astype(bf16)

    left_over = sent.at[pl.ds(0, 127)]
    pltpu.make_async_copy(left_over, left_over, dma.at[0]).wait()
    pl.when(xl != core)(pltpu.make_async_copy(sent.at[0], sent.at[0], dma.at[2]).wait)
    left_over = back.at[pl.ds(0, 126)]
    pltpu.make_async_copy(left_over, left_over, dma.at[5]).wait()
    for half in range(2):
        mine = (xh == core) & (xl == lax.rem(core + half, 2))
        one = pltpu.make_async_copy(back.at[0], back.at[0], dma.at[7 + half])
        pl.when(jnp.logical_not(mine))(one.wait)


def local(pair, norm_in, shift_in, in_weight, norm_out, shift_out, out_weight):
    f32, bf16 = jnp.float32, jnp.bfloat16
    hbm = pl.BlockSpec(memory_space=pltpu.HBM)
    vmem = pl.BlockSpec(memory_space=pltpu.VMEM)
    return pl.pallas_call(
        kernel,
        out_shape=jax.ShapeDtypeStruct((32, 32, 128), bf16),
        in_specs=[hbm] * 7,
        out_specs=vmem,
        scratch_shapes=[
            pltpu.VMEM((1024, 128), bf16),
            pltpu.VMEM((1, 128), f32),
            pltpu.VMEM((1, 128), f32),
            pltpu.VMEM((128, 640), bf16),
            pltpu.VMEM((1, 128), f32),
            pltpu.VMEM((1, 128), f32),
            pltpu.VMEM((128, 128), bf16),
            pltpu.VMEM((32 * PITCH, 128), f32),
            pltpu.VMEM((2048, 128), f32),
            pltpu.VMEM((128, 16, 128), bf16),
            pltpu.VMEM((16, 8, 16, 128), bf16),
            pltpu.VMEM((256, 512), bf16),
            pltpu.VMEM((2, 512, 256), bf16),
            pltpu.VMEM((8, 2, 8, 8, 128), bf16),
            pltpu.VMEM((128, 8, 128), bf16),
            pltpu.VMEM((32, 32, 128), f32),
            pltpu.VMEM((128, 128), f32),
            pltpu.VMEM((128, 128), f32),
            pltpu.VMEM((512, 128), bf16),
            pltpu.SemaphoreType.DMA((9,)),
            pltpu.SemaphoreType.DMA((7,)),
            pltpu.SemaphoreType.REGULAR((16,)),
        ],
        name="triangle",
        compiler_params=pltpu.CompilerParams(collective_id=0, has_side_effects=True),
    )(
        pair.reshape(1024, 128), norm_in.reshape(1, 128), shift_in.reshape(1, 128), in_weight,
        norm_out.reshape(1, 128), shift_out.reshape(1, 128), out_weight,
    )


def solution(mesh):
    in_specs = (P("row", "col", None), P(), P(), P(), P(), P(), P())
    out_specs = P("row", "col", None)
    return jax.shard_map(local, mesh=mesh, in_specs=in_specs, out_specs=out_specs, check_vma=False)
```

```python
import jax
import jax.numpy as jnp
from jax import lax
from jax.experimental import pallas as pl
from jax.experimental.pallas import tpu as pltpu
from jax.sharding import PartitionSpec as P

EPSILON = 1e-05
MESH = pl.DeviceIdType.MESH
PITCH = 40
NT = (((1,), (1,)), ((), ()))
TN = (((0,), (0,)), ((), ()))
Y_STEP = (2, 1, 3, 0)
ORDER = (
    (0, 0), (0, 1), (0, 3), (1, 0), (3, 0), (0, 2), (1, 1), (1, 3),
    (3, 1), (3, 3), (2, 0), (1, 2), (3, 2), (2, 1), (2, 3), (2, 2),
)
LAST = ((1, 0), (3, 0), (0, 3))


def z_step(t):
    return 4 + (1 - 2 * (t % 2)) * ((t + 1) // 2)


def swap_blocks(tiles):
    lane = lax.broadcasted_iota(jnp.int32, tiles[0].shape, 1)
    low, even = lane < 64, lax.rem(lax.div(lane, 32), 2) == 0

    def turn(x, shift):
        return pltpu.roll(x, shift, 1)

    a, b, c, d = tiles
    a, c = jnp.where(low, a, turn(c, 64)), jnp.where(low, turn(a, 64), c)
    b, d = jnp.where(low, b, turn(d, 64)), jnp.where(low, turn(b, 64), d)
    a, b = jnp.where(even, a, turn(b, 32)), jnp.where(even, turn(a, 96), b)
    c, d = jnp.where(even, c, turn(d, 32)), jnp.where(even, turn(c, 96), d)
    return a, b, c, d


def kernel(
    pair_in, norm_in_in, shift_in_in, in_weight_in, norm_out_in, shift_out_in, out_weight_in, out,
    pair, norm_in, shift_in, in_weight, norm_out, shift_out, out_weight,
    normed, staged, sent, landed, left, right, mixed, back, gate, gain, bias, weight,
    dma, load, ready,
):
    f32, bf16 = jnp.float32, jnp.bfloat16
    r, c = lax.axis_index("row"), lax.axis_index("col")
    xh, z = lax.div(r, 8), lax.rem(r, 8)
    xl, y, core = lax.div(c, 8), lax.rem(lax.div(c, 2), 4), lax.rem(c, 2)
    spot = lax.div(c, 2)

    sources = (pair_in, norm_in_in, shift_in_in, in_weight_in, norm_out_in, shift_out_in, out_weight_in)
    places = (pair, norm_in, shift_in, in_weight, norm_out, shift_out, out_weight)
    loads = [pltpu.make_async_copy(f, t, load.at[n]) for n, (f, t) in enumerate(zip(sources, places))]
    for n in (0, 3, 1, 2, 4, 5, 6):
        loads[n].start()

    def line(dx, dy):
        x = lax.rem(2 * xh + xl + dx, 4)
        return lax.div(x, 2), lax.rem(x, 2) * 4 + lax.rem(y + dy, 4)

    def tell(semaphore, R, C):
        pl.semaphore_signal(semaphore, inc=1, device_id=(R, C), device_id_type=MESH)

    barrier = pltpu.get_barrier_semaphore()
    for dx, dy in ((1, 0), (3, 0), (0, 1), (0, 3)):
        H, S = line(dx, dy)
        tell(barrier, H * 8 + z, S * 2 + core)
    for dz in (4, 3, 5, 2, 6, 1, 7):
        for e in range(2):
            tell(barrier, xh * 8 + lax.rem(z + dz, 8), spot * 2 + e)
    tell(barrier, r, spot * 2 + 1 - core)

    for n in (0, 1, 2):
        loads[n].wait()

    def norm_rows(n, _):
        x = pair[pl.ds(n * 128, 128), :].astype(f32)
        center = jnp.mean(x, axis=-1, keepdims=True)
        x = x - center
        spread = jnp.mean(x * x, axis=-1, keepdims=True)
        x = x * lax.rsqrt(spread + EPSILON) * norm_in[...] + shift_in[...]
        for m in range(4):
            normed[pl.ds((n * 4 + m) * PITCH, 32), :] = x[m * 32 : (m + 1) * 32]
        return 0

    lax.fori_loop(0, 8, norm_rows, 0)
    loads[3].wait()
    weight[...] = in_weight[:, :512].astype(f32).T.astype(bf16)

    def glu(rows, x):
        p = lax.dot_general(weight[pl.ds(rows, 256), :], x, NT, preferred_element_type=f32)
        return jax.nn.sigmoid(p[:128]) * p[128:]

    for s in range(0, 8, 2):
        parts = [normed[pl.ds(b * 8 + s + e, 32, stride=PITCH), :] for e in range(2) for b in range(4)]
        value = glu(0, jnp.concatenate(parts, axis=0).astype(bf16))
        for e in range(2):
            staged[pl.ds(s + e, 128, stride=16), :] = value[:, e * 128 : (e + 1) * 128]
        parts = [normed[pl.ds((b * 8 + s + e) * PITCH, 32), :] for e in range(2) for b in range(4)]
        value = glu(256, jnp.concatenate(parts, axis=0).astype(bf16))
        for e in range(2):
            staged[pl.ds(8 + s + e, 128, stride=16), :] = value[:, e * 128 : (e + 1) * 128]

    def pack(n, _):
        sent[pl.ds(n * 16, 16)] = staged[pl.ds(n * 256, 256), :].astype(bf16).reshape(16, 16, 128)
        return 0

    lax.fori_loop(0, 8, pack, 0)

    def inward(R, S, send):
        return pltpu.make_async_remote_copy(
            src_ref=sent.at[R * 8 + S], dst_ref=landed.at[r, lax.rem(c, 8)], send_sem=dma.at[send],
            recv_sem=dma.at[1], device_id=(R, S * 2 + xl), device_id_type=MESH,
        )

    def send_line(dx, dy):
        H, S = line(dx, dy)

        def go_in(t, _):
            inward(H * 8 + lax.rem(z + z_step(t), 8), S, 0).start()
            return 0

        lax.fori_loop(0, 7 if (dx, dy) == (0, 0) else 8, go_in, 0, unroll=True)
        if (dx, dy) == (0, 0):
            own_in = pltpu.make_async_copy(sent.at[r * 8 + spot], landed.at[r, lax.rem(c, 8)], dma.at[1])
            pl.when(xl == core)(own_in.start)
            pl.when(xl != core)(inward(r, spot, 2).start)

    pl.semaphore_wait(barrier, 19)
    for dx, dy in ORDER:
        if (dx, dy) != (0, 0):
            pl.semaphore_wait(ready.at[dx * 4 + dy], 1)

        def pass_on(ex, ey, dx=dx, dy=dy):
            h, s = line(ex, ey)
            tell(ready.at[(dx - ex) % 4 * 4 + (dy - ey) % 4], h * 8 + z, s * 2 + core)

        if dx == 0:
            if dy in (0, 1):
                pass_on(0, 3)
            if dy == 0:
                pass_on(0, 1)
            pass_on(3, 0)
            pass_on(1, 0)
        if dx == 1:
            pass_on(3, 0)

        if (dx, dy) not in LAST:
            send_line(dx, dy)
    for dx, dy in LAST:
        send_line(dx, dy)

    def gate_rows(n, _):
        parts = [normed[pl.ds((n * 4 + m) * PITCH, 32), :] for m in range(4)]
        x = jnp.concatenate(parts, axis=0).astype(bf16)
        p = jnp.dot(x, in_weight[:, 512:], preferred_element_type=f32)
        gate[pl.ds(n * 4, 4)] = jax.nn.sigmoid(p).reshape(4, 32, 128)
        return 0

    lax.fori_loop(0, 8, gate_rows, 0)
    for n in (4, 5, 6):
        loads[n].wait()
    gain[...] = jnp.broadcast_to(norm_out[...], (128, 128)).T
    bias[...] = jnp.broadcast_to(shift_out[...], (128, 128)).T

    pltpu.make_async_copy(landed, landed, dma.at[1]).wait()

    for q in range(2):
        tiles = [landed[:, q * 4 + n].astype(f32)[:, 8:].reshape(128, 128) for n in range(4)]
        tiles = [t.reshape(16, 1, 8, 128) for t in swap_blocks(tiles)]
        block = jnp.concatenate(tiles, axis=1).reshape(512, 128)
        right[0, :, q * 128 : (q + 1) * 128] = block.astype(bf16)
    for n in range(8):
        tiles = landed[:, n].astype(f32)[:, :8].reshape(4, 4, 8, 128)
        tiles = swap_blocks([tiles[:, m].reshape(32, 128) for m in range(4)])
        for m in range(4):
            block = jnp.concatenate([t[m * 8 : (m + 1) * 8] for t in tiles], axis=0)
            left[n * 32 : (n + 1) * 32, m * 128 : (m + 1) * 128] = block.astype(bf16)

    swap = pltpu.make_async_remote_copy(
        src_ref=right.at[0], dst_ref=right.at[1], send_sem=dma.at[3], recv_sem=dma.at[4],
        device_id=(r, spot * 2 + 1 - core), device_id_type=MESH,
    )
    swap.start()

    def outward(R, C, half, send):
        return pltpu.make_async_remote_copy(
            src_ref=mixed.at[lax.rem(R, 8), half, lax.rem(C, 8)], dst_ref=back.at[r * 8 + spot],
            send_sem=dma.at[send], recv_sem=dma.at[6], device_id=(R, C), device_id_type=MESH,
        )

    for half in range(2):
        if half == 1:
            swap.wait()
        product = jnp.dot(left[...], right[half], preferred_element_type=f32)
        for q in range(2):
            tiles = product[:, q * 128 : (q + 1) * 128].reshape(8, 4, 8, 128)
            tiles = swap_blocks([tiles[:, m].reshape(64, 128) for m in range(4)])
            for m in range(4):
                mixed[:, half, q * 4 + m] = tiles[m].reshape(8, 8, 128).astype(bf16)
        X = lax.rem(core + half, 2)

        for u in range(4):
            far = X * 8 + lax.rem(y + Y_STEP[u], 4) * 2

            def go_out(t, _, half=half, far=far):
                R = core * 8 + lax.rem(z + z_step(t), 8)
                for e in range(2):
                    outward(R, far + e, half, 5).start()
                return 0

            lax.fori_loop(0, 7 if u == 3 else 8, go_out, 0, unroll=True)
        R, C = core * 8 + z, X * 8 + y * 2
        outward(R, C + 1 - core, half, 5).start()
        mine = (xh == core) & (xl == X)
        own_out = pltpu.make_async_copy(
            mixed.at[z, half, lax.rem(c, 8)], back.at[r * 8 + spot], dma.at[6]
        )
        pl.when(mine)(own_out.start)
        pl.when(jnp.logical_not(mine))(outward(R, C + core, half, 7 + half).start)

    pltpu.make_async_copy(back, back, dma.at[6]).wait()

    def total(n, s):
        return s + jnp.sum(back[pl.ds(n * 16, 16)].astype(f32), axis=0)

    center = lax.fori_loop(0, 8, total, jnp.zeros((8, 128), f32)) / 128

    def square(n, s):
        x = back[pl.ds(n * 16, 16)].astype(f32) - center[None]
        return s + jnp.sum(x * x, axis=0)

    scale = lax.rsqrt(lax.fori_loop(0, 8, square, jnp.zeros((8, 128), f32)) / 128 + EPSILON)

    def rescale(n, _):
        x = (back[pl.ds(n * 16, 16)].astype(f32) - center[None]) * scale[None]
        staged[pl.ds(n * 128, 128), :] = x.reshape(128, 128)
        return 0

    lax.fori_loop(0, 8, rescale, 0)
    for s in range(8):
        x = staged[pl.ds(s, 128, stride=8), :] * gain[...] + bias[...]
        x = lax.dot_general(x.astype(bf16), out_weight[...], TN, preferred_element_type=f32)
        for b in range(4):
            out[b * 8 + s] = (gate[b * 8 + s] * x[b * 32 : (b + 1) * 32]).astype(bf16)

    left_over = sent.at[pl.ds(0, 127)]
    pltpu.make_async_copy(left_over, left_over, dma.at[0]).wait()
    pl.when(xl != core)(pltpu.make_async_copy(sent.at[0], sent.at[0], dma.at[2]).wait)
    left_over = back.at[pl.ds(0, 126)]
    pltpu.make_async_copy(left_over, left_over, dma.at[5]).wait()
    for half in range(2):
        mine = (xh == core) & (xl == lax.rem(core + half, 2))
        one = pltpu.make_async_copy(back.at[0], back.at[0], dma.at[7 + half])
        pl.when(jnp.logical_not(mine))(one.wait)


def local(pair, norm_in, shift_in, in_weight, norm_out, shift_out, out_weight):
    f32, bf16 = jnp.float32, jnp.bfloat16
    hbm = pl.BlockSpec(memory_space=pltpu.HBM)
    vmem = pl.BlockSpec(memory_space=pltpu.VMEM)
    return pl.pallas_call(
        kernel,
        out_shape=pltpu.VMEM((32, 32, 128), bf16),
        in_specs=[hbm] * 7,
        out_specs=vmem,
        scratch_shapes=[
            pltpu.VMEM((1024, 128), bf16),
            pltpu.VMEM((1, 128), f32),
            pltpu.VMEM((1, 128), f32),
            pltpu.VMEM((128, 640), bf16),
            pltpu.VMEM((1, 128), f32),
            pltpu.VMEM((1, 128), f32),
            pltpu.VMEM((128, 128), bf16),
            pltpu.VMEM((32 * PITCH, 128), f32),
            pltpu.VMEM((2048, 128), f32),
            pltpu.VMEM((128, 16, 128), bf16),
            pltpu.VMEM((16, 8, 16, 128), bf16),
            pltpu.VMEM((256, 512), bf16),
            pltpu.VMEM((2, 512, 256), bf16),
            pltpu.VMEM((8, 2, 8, 8, 128), bf16),
            pltpu.VMEM((128, 8, 128), bf16),
            pltpu.VMEM((32, 32, 128), f32),
            pltpu.VMEM((128, 128), f32),
            pltpu.VMEM((128, 128), f32),
            pltpu.VMEM((512, 128), bf16),
            pltpu.SemaphoreType.DMA((9,)),
            pltpu.SemaphoreType.DMA((7,)),
            pltpu.SemaphoreType.REGULAR((16,)),
        ],
        name="triangle",
        compiler_params=pltpu.CompilerParams(collective_id=0, has_side_effects=True),
    )(
        pair.reshape(1024, 128), norm_in.reshape(1, 128), shift_in.reshape(1, 128), in_weight,
        norm_out.reshape(1, 128), shift_out.reshape(1, 128), out_weight,
    )


def solution(mesh):
    in_specs = (P("row", "col", None), P(), P(), P(), P(), P(), P())
    out_specs = P("row", "col", None)
    return jax.shard_map(local, mesh=mesh, in_specs=in_specs, out_specs=out_specs, check_vma=False)
```

```python
import jax
import jax.numpy as jnp
from jax import lax
from jax.experimental import pallas as pl
from jax.experimental.pallas import tpu as pltpu
from jax.sharding import PartitionSpec as P

EPSILON = 1e-05
MESH = pl.DeviceIdType.MESH
PITCH = 40
NT = (((1,), (1,)), ((), ()))
TN = (((0,), (0,)), ((), ()))
Y_STEP = (2, 1, 3, 0)
ORDER = (
    (0, 0), (0, 1), (0, 3), (1, 0), (3, 0), (0, 2), (1, 1), (1, 3),
    (3, 1), (3, 3), (2, 0), (1, 2), (3, 2), (2, 1), (2, 3), (2, 2),
)
LAST = ((1, 0), (3, 0), (0, 3))


def z_step(t):
    return 4 + (1 - 2 * (t % 2)) * ((t + 1) // 2)


def swap_blocks(tiles):
    lane = lax.broadcasted_iota(jnp.int32, tiles[0].shape, 1)
    low, even = lane < 64, lax.rem(lax.div(lane, 32), 2) == 0

    def turn(x, shift):
        return pltpu.roll(x, shift, 1)

    a, b, c, d = tiles
    a, c = jnp.where(low, a, turn(c, 64)), jnp.where(low, turn(a, 64), c)
    b, d = jnp.where(low, b, turn(d, 64)), jnp.where(low, turn(b, 64), d)
    a, b = jnp.where(even, a, turn(b, 32)), jnp.where(even, turn(a, 96), b)
    c, d = jnp.where(even, c, turn(d, 32)), jnp.where(even, turn(c, 96), d)
    return a, b, c, d


def kernel(
    pair_in, norm_in_in, shift_in_in, in_weight_in, norm_out_in, shift_out_in, out_weight_in, out,
    pair, norm_in, shift_in, in_weight, norm_out, shift_out, out_weight,
    normed, staged, sent, landed, left, right, mixed, back, gate, gain, bias, weight,
    dma, load, ready,
):
    f32, bf16 = jnp.float32, jnp.bfloat16
    r, c = lax.axis_index("row"), lax.axis_index("col")
    xh, z = lax.div(r, 8), lax.rem(r, 8)
    xl, y, core = lax.div(c, 8), lax.rem(lax.div(c, 2), 4), lax.rem(c, 2)
    spot = lax.div(c, 2)

    sources = (pair_in, norm_in_in, shift_in_in, in_weight_in, norm_out_in, shift_out_in, out_weight_in)
    places = (pair, norm_in, shift_in, in_weight, norm_out, shift_out, out_weight)
    loads = [pltpu.make_async_copy(f, t, load.at[n]) for n, (f, t) in enumerate(zip(sources, places))]
    for n in (0, 3, 1, 2, 4, 5, 6):
        loads[n].start()

    def line(dx, dy):
        x = lax.rem(2 * xh + xl + dx, 4)
        return lax.div(x, 2), lax.rem(x, 2) * 4 + lax.rem(y + dy, 4)

    def tell(semaphore, R, C):
        pl.semaphore_signal(semaphore, inc=1, device_id=(R, C), device_id_type=MESH)

    barrier = pltpu.get_barrier_semaphore()
    for dx, dy in ((1, 0), (3, 0), (0, 1), (0, 3)):
        H, S = line(dx, dy)
        tell(barrier, H * 8 + z, S * 2 + core)
    for dz in (4, 3, 5, 2, 6, 1, 7):
        for e in range(2):
            tell(barrier, xh * 8 + lax.rem(z + dz, 8), spot * 2 + e)
    tell(barrier, r, spot * 2 + 1 - core)

    for n in (0, 1, 2):
        loads[n].wait()

    def norm_rows(n, _):
        x = pair[pl.ds(n * 128, 128), :].astype(f32)
        center = jnp.mean(x, axis=-1, keepdims=True)
        x = x - center
        spread = jnp.mean(x * x, axis=-1, keepdims=True)
        x = x * lax.rsqrt(spread + EPSILON) * norm_in[...] + shift_in[...]
        for m in range(4):
            normed[pl.ds((n * 4 + m) * PITCH, 32), :] = x[m * 32 : (m + 1) * 32]
        return 0

    lax.fori_loop(0, 8, norm_rows, 0)
    loads[3].wait()
    weight[...] = in_weight[:, :512].astype(f32).T.astype(bf16)

    def glu(rows, x):
        p = lax.dot_general(weight[pl.ds(rows, 256), :], x, NT, preferred_element_type=f32)
        return jax.nn.sigmoid(p[:128]) * p[128:]

    for s in range(0, 8, 2):
        parts = [normed[pl.ds(b * 8 + s + e, 32, stride=PITCH), :] for e in range(2) for b in range(4)]
        value = glu(0, jnp.concatenate(parts, axis=0).astype(bf16))
        for e in range(2):
            staged[pl.ds(s + e, 128, stride=16), :] = value[:, e * 128 : (e + 1) * 128]
        parts = [normed[pl.ds((b * 8 + s + e) * PITCH, 32), :] for e in range(2) for b in range(4)]
        value = glu(256, jnp.concatenate(parts, axis=0).astype(bf16))
        for e in range(2):
            staged[pl.ds(8 + s + e, 128, stride=16), :] = value[:, e * 128 : (e + 1) * 128]

    def pack(n, _):
        sent[pl.ds(n * 16, 16)] = staged[pl.ds(n * 256, 256), :].astype(bf16).reshape(16, 16, 128)
        return 0

    lax.fori_loop(0, 8, pack, 0)

    arrived = dma.at[1 + 8 * lax.div(y, 2)]

    def inward(R, S, send):
        return pltpu.make_async_remote_copy(
            src_ref=sent.at[R * 8 + S], dst_ref=landed.at[r, lax.rem(c, 8)], send_sem=dma.at[send],
            recv_sem=arrived, device_id=(R, S * 2 + xl), device_id_type=MESH,
        )

    def send_line(dx, dy):
        H, S = line(dx, dy)

        def go_in(t, _):
            inward(H * 8 + lax.rem(z + z_step(t), 8), S, 0).start()
            return 0

        lax.fori_loop(0, 7 if (dx, dy) == (0, 0) else 8, go_in, 0, unroll=True)
        if (dx, dy) == (0, 0):
            own_in = pltpu.make_async_copy(sent.at[r * 8 + spot], landed.at[r, lax.rem(c, 8)], arrived)
            pl.when(xl == core)(own_in.start)
            pl.when(xl != core)(inward(r, spot, 2).start)

    pl.semaphore_wait(barrier, 19)
    for dx, dy in ORDER:
        if (dx, dy) != (0, 0):
            pl.semaphore_wait(ready.at[dx * 4 + dy], 1)

        def pass_on(ex, ey, dx=dx, dy=dy):
            h, s = line(ex, ey)
            tell(ready.at[(dx - ex) % 4 * 4 + (dy - ey) % 4], h * 8 + z, s * 2 + core)

        if dx == 0:
            if dy in (0, 1):
                pass_on(0, 3)
            if dy == 0:
                pass_on(0, 1)
            pass_on(3, 0)
            pass_on(1, 0)
        if dx == 1:
            pass_on(3, 0)

        if (dx, dy) not in LAST:
            send_line(dx, dy)
    for dx, dy in LAST:
        send_line(dx, dy)

    def gate_rows(n, _):
        parts = [normed[pl.ds((n * 4 + m) * PITCH, 32), :] for m in range(4)]
        x = jnp.concatenate(parts, axis=0).astype(bf16)
        p = jnp.dot(x, in_weight[:, 512:], preferred_element_type=f32)
        gate[pl.ds(n * 4, 4)] = jax.nn.sigmoid(p).reshape(4, 32, 128)
        return 0

    lax.fori_loop(0, 8, gate_rows, 0)
    for n in (4, 5, 6):
        loads[n].wait()
    gain[...] = jnp.broadcast_to(norm_out[...], (128, 128)).T
    bias[...] = jnp.broadcast_to(shift_out[...], (128, 128)).T

    def swap(q):
        return pltpu.make_async_remote_copy(
            src_ref=right.at[0, q], dst_ref=right.at[1, q], send_sem=dma.at[3 + 4 * q], recv_sem=dma.at[4 + 4 * q],
            device_id=(r, spot * 2 + 1 - core), device_id_type=MESH,
        )

    def outward(R, C, half):
        return pltpu.make_async_remote_copy(
            src_ref=mixed.at[lax.rem(R, 8), half, lax.rem(C, 8)], dst_ref=back.at[r * 8 + spot],
            send_sem=dma.at[5], recv_sem=dma.at[6], device_id=(R, C), device_id_type=MESH,
        )

    def answer(half, g, q):
        product = jnp.dot(left[g * 128 : (g + 1) * 128], right[half, q], preferred_element_type=f32)
        tiles = product.reshape(4, 4, 8, 128)
        tiles = swap_blocks([tiles[:, m].reshape(32, 128) for m in range(4)])
        for m in range(4):
            mixed[g * 4 : (g + 1) * 4, half, q * 4 + m] = tiles[m].reshape(4, 8, 128).astype(bf16)
        X = lax.rem(core + half, 2)
        for db in (2, 3, 1, 0):
            C = X * 8 + q * 4 + lax.rem(c + db, 4)
            for da in (2, 1, 3, 0):
                R = core * 8 + g * 4 + lax.rem(z + da, 4)
                if da or db:
                    outward(R, C, half).start()
        mine = (xh == core) & (xl == X) & (lax.div(z, 4) == g) & (lax.div(y, 2) == q)
        own_out = pltpu.make_async_copy(mixed.at[z, half, lax.rem(c, 8)], back.at[r * 8 + spot], dma.at[6])
        pl.when(mine)(own_out.start)
        pl.when(jnp.logical_not(mine))(outward(R, C, half).start)

    for q in range(2):
        pltpu.make_async_copy(landed.at[0:8], landed.at[0:8], dma.at[1 + 8 * q]).wait()
        tiles = [landed[:, q * 4 + n].astype(f32)[:, 8:].reshape(128, 128) for n in range(4)]
        tiles = [t.reshape(16, 1, 8, 128) for t in swap_blocks(tiles)]
        right[0, q] = jnp.concatenate(tiles, axis=1).reshape(512, 128).astype(bf16)
        for n in range(q * 4, q * 4 + 4):
            tiles = landed[:, n].astype(f32)[:, :8].reshape(4, 4, 8, 128)
            tiles = swap_blocks([tiles[:, m].reshape(32, 128) for m in range(4)])
            for m in range(4):
                block = jnp.concatenate([t[m * 8 : (m + 1) * 8] for t in tiles], axis=0)
                left[n * 32 : (n + 1) * 32, m * 128 : (m + 1) * 128] = block.astype(bf16)
        swap(q).start()
        for half in range(2):
            if half == 1:
                swap(q).wait()
            for place in ((0, 0),) if q == 0 else ((0, 1), (1, 0), (1, 1)):
                answer(half, *place)

    pltpu.make_async_copy(back, back, dma.at[6]).wait()

    def total(n, s):
        return s + jnp.sum(back[pl.ds(n * 16, 16)].astype(f32), axis=0)

    center = lax.fori_loop(0, 8, total, jnp.zeros((8, 128), f32)) / 128

    def square(n, s):
        x = back[pl.ds(n * 16, 16)].astype(f32) - center[None]
        return s + jnp.sum(x * x, axis=0)

    scale = lax.rsqrt(lax.fori_loop(0, 8, square, jnp.zeros((8, 128), f32)) / 128 + EPSILON)

    def rescale(n, _):
        x = (back[pl.ds(n * 16, 16)].astype(f32) - center[None]) * scale[None]
        staged[pl.ds(n * 128, 128), :] = x.reshape(128, 128)
        return 0

    lax.fori_loop(0, 8, rescale, 0)
    for s in range(8):
        x = staged[pl.ds(s, 128, stride=8), :] * gain[...] + bias[...]
        x = lax.dot_general(x.astype(bf16), out_weight[...], TN, preferred_element_type=f32)
        for b in range(4):
            out[b * 8 + s] = (gate[b * 8 + s] * x[b * 32 : (b + 1) * 32]).astype(bf16)

    left_over = sent.at[pl.ds(0, 127)]
    pltpu.make_async_copy(left_over, left_over, dma.at[0]).wait()
    pl.when(xl != core)(pltpu.make_async_copy(sent.at[0], sent.at[0], dma.at[2]).wait)
    left_over = back.at[pl.ds(0, 127)]
    pl.when(xh == core)(pltpu.make_async_copy(left_over, left_over, dma.at[5]).wait)
    pl.when(xh != core)(pltpu.make_async_copy(back, back, dma.at[5]).wait)


def local(pair, norm_in, shift_in, in_weight, norm_out, shift_out, out_weight):
    f32, bf16 = jnp.float32, jnp.bfloat16
    hbm = pl.BlockSpec(memory_space=pltpu.HBM)
    vmem = pl.BlockSpec(memory_space=pltpu.VMEM)
    return pl.pallas_call(
        kernel,
        out_shape=pltpu.VMEM((32, 32, 128), bf16),
        in_specs=[hbm] * 7,
        out_specs=vmem,
        scratch_shapes=[
            pltpu.VMEM((1024, 128), bf16),
            pltpu.VMEM((1, 128), f32),
            pltpu.VMEM((1, 128), f32),
            pltpu.VMEM((128, 640), bf16),
            pltpu.VMEM((1, 128), f32),
            pltpu.VMEM((1, 128), f32),
            pltpu.VMEM((128, 128), bf16),
            pltpu.VMEM((32 * PITCH, 128), f32),
            pltpu.VMEM((2048, 128), f32),
            pltpu.VMEM((128, 16, 128), bf16),
            pltpu.VMEM((16, 8, 16, 128), bf16),
            pltpu.VMEM((256, 512), bf16),
            pltpu.VMEM((2, 2, 512, 128), bf16),
            pltpu.VMEM((8, 2, 8, 8, 128), bf16),
            pltpu.VMEM((128, 8, 128), bf16),
            pltpu.VMEM((32, 32, 128), f32),
            pltpu.VMEM((128, 128), f32),
            pltpu.VMEM((128, 128), f32),
            pltpu.VMEM((512, 128), bf16),
            pltpu.SemaphoreType.DMA((10,)),
            pltpu.SemaphoreType.DMA((7,)),
            pltpu.SemaphoreType.REGULAR((16,)),
        ],
        name="triangle",
        compiler_params=pltpu.CompilerParams(collective_id=0, has_side_effects=True),
    )(
        pair.reshape(1024, 128), norm_in.reshape(1, 128), shift_in.reshape(1, 128), in_weight,
        norm_out.reshape(1, 128), shift_out.reshape(1, 128), out_weight,
    )


def solution(mesh):
    in_specs = (P("row", "col", None), P(), P(), P(), P(), P(), P())
    out_specs = P("row", "col", None)
    return jax.shard_map(local, mesh=mesh, in_specs=in_specs, out_specs=out_specs, check_vma=False)
```

```python
import jax
import jax.numpy as jnp
from jax import lax
from jax.experimental import pallas as pl
from jax.experimental.pallas import tpu as pltpu
from jax.sharding import PartitionSpec as P

EPSILON = 1e-05
MESH = pl.DeviceIdType.MESH
PITCH = 40
NT = (((1,), (1,)), ((), ()))
TN = (((0,), (0,)), ((), ()))
Y_STEP = (2, 1, 3, 0)
ORDER = (
    (0, 0), (0, 1), (0, 3), (1, 0), (3, 0), (0, 2), (1, 1), (1, 3),
    (3, 1), (3, 3), (2, 0), (1, 2), (3, 2), (2, 1), (2, 3), (2, 2),
)
LAST = ((1, 0), (3, 0), (0, 3))


def z_step(t):
    return 4 + (1 - 2 * (t % 2)) * ((t + 1) // 2)


def swap_blocks(tiles):
    lane = lax.broadcasted_iota(jnp.int32, tiles[0].shape, 1)
    low, even = lane < 64, lax.rem(lax.div(lane, 32), 2) == 0

    def turn(x, shift):
        return pltpu.roll(x, shift, 1)

    a, b, c, d = tiles
    a, c = jnp.where(low, a, turn(c, 64)), jnp.where(low, turn(a, 64), c)
    b, d = jnp.where(low, b, turn(d, 64)), jnp.where(low, turn(b, 64), d)
    a, b = jnp.where(even, a, turn(b, 32)), jnp.where(even, turn(a, 96), b)
    c, d = jnp.where(even, c, turn(d, 32)), jnp.where(even, turn(c, 96), d)
    return a, b, c, d


def kernel(
    pair_in, norm_in_in, shift_in_in, in_weight_in, norm_out_in, shift_out_in, out_weight_in, out,
    pair, norm_in, shift_in, in_weight, norm_out, shift_out, out_weight,
    normed, staged, sent, landed, left, right, mixed, back, gate, gain, bias, weight,
    dma, load, ready,
):
    f32, bf16 = jnp.float32, jnp.bfloat16
    r, c = lax.axis_index("row"), lax.axis_index("col")
    xh, z = lax.div(r, 8), lax.rem(r, 8)
    xl, y, core = lax.div(c, 8), lax.rem(lax.div(c, 2), 4), lax.rem(c, 2)
    spot = lax.div(c, 2)

    sources = (pair_in, norm_in_in, shift_in_in, in_weight_in, norm_out_in, shift_out_in, out_weight_in)
    places = (pair, norm_in, shift_in, in_weight, norm_out, shift_out, out_weight)
    loads = [pltpu.make_async_copy(f, t, load.at[n]) for n, (f, t) in enumerate(zip(sources, places))]
    for n in (3, 0, 1, 2, 4, 5, 6):
        loads[n].start()

    def line(dx, dy):
        x = lax.rem(2 * xh + xl + dx, 4)
        return lax.div(x, 2), lax.rem(x, 2) * 4 + lax.rem(y + dy, 4)

    def tell(semaphore, R, C):
        pl.semaphore_signal(semaphore, inc=1, device_id=(R, C), device_id_type=MESH)

    barrier = pltpu.get_barrier_semaphore()
    for dx, dy in ((1, 0), (3, 0), (0, 1), (0, 3)):
        H, S = line(dx, dy)
        tell(barrier, H * 8 + z, S * 2 + core)
    for dz in (4, 3, 5, 2, 6, 1, 7):
        for e in range(2):
            tell(barrier, xh * 8 + lax.rem(z + dz, 8), spot * 2 + e)
    tell(barrier, r, spot * 2 + 1 - core)

    loads[3].wait()
    weight[...] = in_weight[:, :512].astype(f32).T.astype(bf16)
    for n in (0, 1, 2):
        loads[n].wait()

    def norm_rows(n, _):
        x = pair[pl.ds(n * 128, 128), :].astype(f32)
        center = jnp.mean(x, axis=-1, keepdims=True)
        x = x - center
        spread = jnp.mean(x * x, axis=-1, keepdims=True)
        x = x * lax.rsqrt(spread + EPSILON) * norm_in[...] + shift_in[...]
        for m in range(4):
            normed[pl.ds((n * 4 + m) * PITCH, 32), :] = x[m * 32 : (m + 1) * 32]
        return 0

    lax.fori_loop(0, 8, norm_rows, 0, unroll=2)

    def glu(rows, x):
        p = lax.dot_general(weight[pl.ds(rows, 256), :], x, NT, preferred_element_type=f32)
        return jax.nn.sigmoid(p[:128]) * p[128:]

    for s in range(0, 8, 2):
        parts = [normed[pl.ds(b * 8 + s + e, 32, stride=PITCH), :] for e in range(2) for b in range(4)]
        value = glu(0, jnp.concatenate(parts, axis=0).astype(bf16))
        for e in range(2):
            staged[pl.ds(s + e, 128, stride=16), :] = value[:, e * 128 : (e + 1) * 128]
        parts = [normed[pl.ds((b * 8 + s + e) * PITCH, 32), :] for e in range(2) for b in range(4)]
        value = glu(256, jnp.concatenate(parts, axis=0).astype(bf16))
        for e in range(2):
            staged[pl.ds(8 + s + e, 128, stride=16), :] = value[:, e * 128 : (e + 1) * 128]

    def pack(n, _):
        sent[pl.ds(n * 16, 16)] = staged[pl.ds(n * 256, 256), :].astype(bf16).reshape(16, 16, 128)
        return 0

    lax.fori_loop(0, 8, pack, 0, unroll=4)

    arrived = dma.at[1 + 8 * lax.div(y, 2)]

    def inward(R, S, send):
        return pltpu.make_async_remote_copy(
            src_ref=sent.at[R * 8 + S], dst_ref=landed.at[r, lax.rem(c, 8)], send_sem=dma.at[send],
            recv_sem=arrived, device_id=(R, S * 2 + xl), device_id_type=MESH,
        )

    def send_line(dx, dy):
        H, S = line(dx, dy)

        def go_in(t, _):
            inward(H * 8 + lax.rem(z + z_step(t), 8), S, 0).start()
            return 0

        lax.fori_loop(0, 7 if (dx, dy) == (0, 0) else 8, go_in, 0, unroll=True)
        if (dx, dy) == (0, 0):
            own_in = pltpu.make_async_copy(sent.at[r * 8 + spot], landed.at[r, lax.rem(c, 8)], arrived)
            pl.when(xl == core)(own_in.start)
            pl.when(xl != core)(inward(r, spot, 2).start)

    pl.semaphore_wait(barrier, 19)
    for dx, dy in ORDER:
        if (dx, dy) != (0, 0):
            pl.semaphore_wait(ready.at[dx * 4 + dy], 1)

        def pass_on(ex, ey, dx=dx, dy=dy):
            h, s = line(ex, ey)
            tell(ready.at[(dx - ex) % 4 * 4 + (dy - ey) % 4], h * 8 + z, s * 2 + core)

        if dx == 0:
            if dy in (0, 1):
                pass_on(0, 3)
            if dy == 0:
                pass_on(0, 1)
            pass_on(3, 0)
            pass_on(1, 0)
        if dx == 1:
            pass_on(3, 0)

        if (dx, dy) not in LAST:
            send_line(dx, dy)
    for dx, dy in LAST:
        send_line(dx, dy)

    def gate_rows(n, _):
        parts = [normed[pl.ds((n * 4 + m) * PITCH, 32), :] for m in range(4)]
        x = jnp.concatenate(parts, axis=0).astype(bf16)
        p = jnp.dot(x, in_weight[:, 512:], preferred_element_type=f32)
        gate[pl.ds(n * 4, 4)] = jax.nn.sigmoid(p).reshape(4, 32, 128)
        return 0

    lax.fori_loop(0, 8, gate_rows, 0)
    for n in (4, 5, 6):
        loads[n].wait()
    gain[...] = jnp.broadcast_to(norm_out[...], (128, 128)).T
    bias[...] = jnp.broadcast_to(shift_out[...], (128, 128)).T

    def swap(q):
        return pltpu.make_async_remote_copy(
            src_ref=right.at[0, q], dst_ref=right.at[1, q], send_sem=dma.at[3 + 4 * q], recv_sem=dma.at[4 + 4 * q],
            device_id=(r, spot * 2 + 1 - core), device_id_type=MESH,
        )

    def outward(R, C, half):
        return pltpu.make_async_remote_copy(
            src_ref=mixed.at[lax.rem(R, 8), half, lax.rem(C, 8)], dst_ref=back.at[r * 8 + spot],
            send_sem=dma.at[5], recv_sem=dma.at[6], device_id=(R, C), device_id_type=MESH,
        )

    def answer(half, g, q):
        product = jnp.dot(left[g * 128 : (g + 1) * 128], right[half, q], preferred_element_type=f32)
        tiles = product.reshape(4, 4, 8, 128)
        tiles = swap_blocks([tiles[:, m].reshape(32, 128) for m in range(4)])
        for m in range(4):
            mixed[g * 4 : (g + 1) * 4, half, q * 4 + m] = tiles[m].reshape(4, 8, 128).astype(bf16)
        X = lax.rem(core + half, 2)
        for db in (2, 3, 1, 0):
            C = X * 8 + q * 4 + lax.rem(c + db, 4)
            for da in (2, 1, 3, 0):
                R = core * 8 + g * 4 + lax.rem(z + da, 4)
                if da or db:
                    outward(R, C, half).start()
        mine = (xh == core) & (xl == X) & (lax.div(z, 4) == g) & (lax.div(y, 2) == q)
        own_out = pltpu.make_async_copy(mixed.at[z, half, lax.rem(c, 8)], back.at[r * 8 + spot], dma.at[6])
        pl.when(mine)(own_out.start)
        pl.when(jnp.logical_not(mine))(outward(R, C, half).start)

    for q in range(2):
        pltpu.make_async_copy(landed.at[0:8], landed.at[0:8], dma.at[1 + 8 * q]).wait()
        tiles = [landed[:, q * 4 + n].astype(f32)[:, 8:].reshape(128, 128) for n in range(4)]
        tiles = [t.reshape(16, 1, 8, 128) for t in swap_blocks(tiles)]
        right[0, q] = jnp.concatenate(tiles, axis=1).reshape(512, 128).astype(bf16)
        for n in range(q * 4, q * 4 + 4):
            tiles = landed[:, n].astype(f32)[:, :8].reshape(4, 4, 8, 128)
            tiles = swap_blocks([tiles[:, m].reshape(32, 128) for m in range(4)])
            for m in range(4):
                block = jnp.concatenate([t[m * 8 : (m + 1) * 8] for t in tiles], axis=0)
                left[n * 32 : (n + 1) * 32, m * 128 : (m + 1) * 128] = block.astype(bf16)
        swap(q).start()
        for half in range(2):
            if half == 1:
                swap(q).wait()
            for place in ((0, 0),) if q == 0 else ((0, 1), (1, 0), (1, 1)):
                answer(half, *place)

    pltpu.make_async_copy(back, back, dma.at[6]).wait()

    def total(n, s):
        return s + jnp.sum(back[pl.ds(n * 16, 16)].astype(f32), axis=0)

    center = lax.fori_loop(0, 8, total, jnp.zeros((8, 128), f32), unroll=4) / 128

    def square(n, s):
        x = back[pl.ds(n * 16, 16)].astype(f32) - center[None]
        return s + jnp.sum(x * x, axis=0)

    scale = lax.rsqrt(lax.fori_loop(0, 8, square, jnp.zeros((8, 128), f32), unroll=4) / 128 + EPSILON)

    def rescale(n, _):
        x = (back[pl.ds(n * 16, 16)].astype(f32) - center[None]) * scale[None]
        staged[pl.ds(n * 128, 128), :] = x.reshape(128, 128)
        return 0

    lax.fori_loop(0, 8, rescale, 0, unroll=4)
    for s in range(8):
        x = staged[pl.ds(s, 128, stride=8), :] * gain[...] + bias[...]
        x = lax.dot_general(x.astype(bf16), out_weight[...], TN, preferred_element_type=f32)
        for b in range(4):
            out[b * 8 + s] = (gate[b * 8 + s] * x[b * 32 : (b + 1) * 32]).astype(bf16)

    left_over = sent.at[pl.ds(0, 127)]
    pltpu.make_async_copy(left_over, left_over, dma.at[0]).wait()
    pl.when(xl != core)(pltpu.make_async_copy(sent.at[0], sent.at[0], dma.at[2]).wait)
    left_over = back.at[pl.ds(0, 127)]
    pl.when(xh == core)(pltpu.make_async_copy(left_over, left_over, dma.at[5]).wait)
    pl.when(xh != core)(pltpu.make_async_copy(back, back, dma.at[5]).wait)


def local(pair, norm_in, shift_in, in_weight, norm_out, shift_out, out_weight):
    f32, bf16 = jnp.float32, jnp.bfloat16
    hbm = pl.BlockSpec(memory_space=pltpu.HBM)
    vmem = pl.BlockSpec(memory_space=pltpu.VMEM)
    return pl.pallas_call(
        kernel,
        out_shape=pltpu.VMEM((32, 32, 128), bf16),
        in_specs=[hbm] * 7,
        out_specs=vmem,
        scratch_shapes=[
            pltpu.VMEM((1024, 128), bf16),
            pltpu.VMEM((1, 128), f32),
            pltpu.VMEM((1, 128), f32),
            pltpu.VMEM((128, 640), bf16),
            pltpu.VMEM((1, 128), f32),
            pltpu.VMEM((1, 128), f32),
            pltpu.VMEM((128, 128), bf16),
            pltpu.VMEM((33 * PITCH, 128), f32),
            pltpu.VMEM((2064, 128), f32),
            pltpu.VMEM((128, 16, 128), bf16),
            pltpu.VMEM((16, 8, 16, 128), bf16),
            pltpu.VMEM((256, 512), bf16),
            pltpu.VMEM((2, 2, 512, 128), bf16),
            pltpu.VMEM((8, 2, 8, 8, 128), bf16),
            pltpu.VMEM((128, 8, 128), bf16),
            pltpu.VMEM((32, 32, 128), f32),
            pltpu.VMEM((128, 128), f32),
            pltpu.VMEM((128, 128), f32),
            pltpu.VMEM((512, 128), bf16),
            pltpu.SemaphoreType.DMA((10,)),
            pltpu.SemaphoreType.DMA((7,)),
            pltpu.SemaphoreType.REGULAR((16,)),
        ],
        name="triangle",
        compiler_params=pltpu.CompilerParams(collective_id=0, has_side_effects=True),
    )(
        pair.reshape(1024, 128), norm_in.reshape(1, 128), shift_in.reshape(1, 128), in_weight,
        norm_out.reshape(1, 128), shift_out.reshape(1, 128), out_weight,
    )


def solution(mesh):
    in_specs = (P("row", "col", None), P(), P(), P(), P(), P(), P())
    out_specs = P("row", "col", None)
    return jax.shard_map(local, mesh=mesh, in_specs=in_specs, out_specs=out_specs, check_vma=False)
```
